8 devices in a mesh: data: 1 (over z), cp: 8 (over y, x, core).
Axes of the slice: x: 2, y: 2, z: 1, core: 2. Of those that a mesh axis runs over, the one named last changes fastest.
Arguments:
- x_tokens: bfloat16 [16, 2048, 5120], P('data', 'cp')
- positions: int32 [16, 2048], P('data', 'cp')
- w_query: bfloat16 [5120, 5120], replicated
- w_key: bfloat16 [5120, 1024], replicated
- w_value: bfloat16 [5120, 1024], replicated
- w_out: bfloat16 [5120, 5120], replicated
Outputs:
- output: bfloat16 [16, 2048, 5120], P('data', 'cp')
All inputs are finite; a program needn't handle non-finite values.
Results may differ from the reference program's by a relative error of at most 0.00471873.
Values are sent between devices in bfloat16 or wider.
A program may use at most 1 GiB of HBM per device.

```python
import jax
import jax.numpy as jnp
from jax import lax

BATCH_PART = 16
SEQ_LEN = 2048
CP_SIZE = 8
MODEL_DIM = 5120
Q_HEADS = 40
KV_HEADS = 8
HEAD_DIM = 128
ROPE_BASE = 500000
WALK_SEG = 16

GROUP_SIZE = Q_HEADS // KV_HEADS
HALF_LEN = SEQ_LEN // (2 * CP_SIZE)
BLOCK_LEN = min(HALF_LEN, 256)
BLOCK_COUNT = SEQ_LEN // BLOCK_LEN


def to_stored_order(seq_arr):
    tail_dims = seq_arr.shape[2:]
    blocks = seq_arr.reshape((BATCH_PART, 2 * CP_SIZE, HALF_LEN) + tail_dims)
    front_part = blocks[:, :CP_SIZE]
    back_part = jnp.flip(blocks[:, CP_SIZE:], axis=1)
    return jnp.stack([front_part, back_part], axis=2).reshape(seq_arr.shape)


def setup_inputs(seed: int = 0, part: int = 0) -> dict:
    root_key = jax.random.key(seed)
    k_query, k_key, k_value, k_out, k_part = jax.random.split(root_key, 5)
    part_key = jax.random.fold_in(k_part, part)
    k_noise, k_mean, k_walk, k_gap, k_start = jax.random.split(part_key, 5)
    seg_count = SEQ_LEN // WALK_SEG
    walk_steps = jax.random.normal(k_walk, (BATCH_PART, seg_count, MODEL_DIM), jnp.float32)
    walk_path = jnp.repeat(jnp.cumsum(walk_steps, axis=1) * (seg_count ** -0.5), WALK_SEG, axis=1)
    row_mean = jax.random.normal(k_mean, (BATCH_PART, 1, MODEL_DIM), jnp.float32)
    token_noise = jax.random.normal(k_noise, (BATCH_PART, SEQ_LEN, MODEL_DIM), jnp.float32)
    x_seq = 0.5 * token_noise + 0.5 * row_mean + walk_path
    pos_gaps = jax.random.randint(k_gap, (BATCH_PART, SEQ_LEN), 1, 4, dtype=jnp.int32)
    start_pos = jax.random.randint(k_start, (BATCH_PART, 1), 0, 1024, dtype=jnp.int32)
    pos_seq = start_pos + jnp.cumsum(pos_gaps, axis=1, dtype=jnp.int32)
    q_cols = Q_HEADS * HEAD_DIM
    kv_cols = KV_HEADS * HEAD_DIM
    w_query = (jax.random.normal(k_query, (MODEL_DIM, q_cols), jnp.float32) * MODEL_DIM ** -0.5).astype(jnp.bfloat16)
    w_key = (jax.random.normal(k_key, (MODEL_DIM, kv_cols), jnp.float32) * MODEL_DIM ** -0.5).astype(jnp.bfloat16)
    w_value = (jax.random.normal(k_value, (MODEL_DIM, kv_cols), jnp.float32) * MODEL_DIM ** -0.5).astype(jnp.bfloat16)
    w_out = (jax.random.normal(k_out, (q_cols, MODEL_DIM), jnp.float32) * (2.0 * q_cols ** -0.5)).astype(jnp.bfloat16)
    return {'x_tokens': to_stored_order(x_seq).astype(jnp.bfloat16), 'positions': to_stored_order(pos_seq), 'w_query': w_query, 'w_key': w_key, 'w_value': w_value, 'w_out': w_out}


def apply_rope(head_vecs, positions):
    half_dim = HEAD_DIM // 2
    inv_freq = 1.0 / (ROPE_BASE ** (jnp.arange(0, HEAD_DIM, 2, dtype=jnp.float32) / HEAD_DIM))
    angles = positions.astype(jnp.float32)[:, :, None] * inv_freq
    tab_shape = angles.shape[:2] + (1,) * (head_vecs.ndim - 3) + (half_dim,)
    cosine = jnp.cos(angles).reshape(tab_shape)
    sine_tab = jnp.sin(angles).reshape(tab_shape)
    lower_half = head_vecs[..., :half_dim].astype(jnp.float32)
    upper_half = head_vecs[..., half_dim:].astype(jnp.float32)
    rotated = jnp.concatenate([lower_half * cosine - upper_half * sine_tab, upper_half * cosine + lower_half * sine_tab], axis=-1)
    return rotated.astype(jnp.bfloat16)


def reference(x_tokens, positions, w_query, w_key, w_value, w_out):
    score_scale = HEAD_DIM ** -0.5
    mask_fill = -1e30
    flat_x = x_tokens.reshape(BATCH_PART * SEQ_LEN, MODEL_DIM)
    q_proj = jnp.dot(flat_x, w_query, preferred_element_type=jnp.float32).astype(jnp.bfloat16)
    k_proj = jnp.dot(flat_x, w_key, preferred_element_type=jnp.float32).astype(jnp.bfloat16)
    v_proj = jnp.dot(flat_x, w_value, preferred_element_type=jnp.float32).astype(jnp.bfloat16)
    q_rot = apply_rope(q_proj.reshape(BATCH_PART, SEQ_LEN, KV_HEADS, GROUP_SIZE, HEAD_DIM), positions)
    k_rot = apply_rope(k_proj.reshape(BATCH_PART, SEQ_LEN, KV_HEADS, HEAD_DIM), positions)
    v_rows = v_proj.reshape(BATCH_PART, SEQ_LEN, KV_HEADS, HEAD_DIM)
    q_blocks = jnp.moveaxis(q_rot.reshape(BATCH_PART, BLOCK_COUNT, BLOCK_LEN, KV_HEADS, GROUP_SIZE, HEAD_DIM), 1, 0)
    k_blocks = jnp.moveaxis(k_rot.reshape(BATCH_PART, BLOCK_COUNT, BLOCK_LEN, KV_HEADS, HEAD_DIM), 1, 0)
    v_blocks = jnp.moveaxis(v_rows.reshape(BATCH_PART, BLOCK_COUNT, BLOCK_LEN, KV_HEADS, HEAD_DIM), 1, 0)
    pos_blocks = jnp.moveaxis(positions.reshape(BATCH_PART, BLOCK_COUNT, BLOCK_LEN), 1, 0)

    def query_block(block_in):
        q_blk, q_pos = block_in
        q_wide = q_blk.astype(jnp.float32)

        def key_step(carry_state, key_in):
            m_run, l_run, acc_run = carry_state
            k_blk, v_blk, k_pos = key_in
            scores = jnp.einsum('bqhgd,bkhd->bhgqk', q_wide, k_blk.astype(jnp.float32)) * score_scale
            allowed = (k_pos[:, None, :] <= q_pos[:, :, None])[:, None, None]
            scores = jnp.where(allowed, scores, mask_fill)
            m_new = jnp.maximum(m_run, jnp.max(scores, axis=-1))
            exp_w = jnp.where(allowed, jnp.exp(scores - m_new[..., None]), 0.0)
            rescale = jnp.exp(m_run - m_new)
            l_new = rescale * l_run + jnp.sum(exp_w, axis=-1)
            pv_part = jnp.einsum('bhgqk,bkhd->bhgqd', exp_w.astype(jnp.bfloat16).astype(jnp.float32), v_blk.astype(jnp.float32))
            return (m_new, l_new, rescale[..., None] * acc_run + pv_part), None

        state_shape = (BATCH_PART, KV_HEADS, GROUP_SIZE, BLOCK_LEN)
        init_state = (jnp.full(state_shape, mask_fill, jnp.float32), jnp.zeros(state_shape, jnp.float32), jnp.zeros(state_shape + (HEAD_DIM,), jnp.float32))
        final_state, _ = lax.scan(key_step, init_state, (k_blocks, v_blocks, pos_blocks))
        attn_out = (final_state[2] / final_state[1][..., None]).astype(jnp.bfloat16)
        return attn_out.transpose(0, 3, 1, 2, 4)

    attn_all = lax.map(query_block, (q_blocks, pos_blocks))
    attn_rows = jnp.moveaxis(attn_all, 0, 1).reshape(BATCH_PART * SEQ_LEN, Q_HEADS * HEAD_DIM)
    out_proj = jnp.dot(attn_rows, w_out, preferred_element_type=jnp.float32).reshape(BATCH_PART, SEQ_LEN, MODEL_DIM)
    return (x_tokens.astype(jnp.float32) + out_proj).astype(jnp.bfloat16)
```

```python
import functools
import math

import jax
import jax.numpy as jnp
from jax import lax
from jax.experimental import pallas as pl
from jax.experimental.pallas import tpu as pltpu
from jax.sharding import PartitionSpec as P

HEAD_DIM = 128
ROPE_BASE = 500000
MASK_FILL = -1e30
SCALE_LOG2 = HEAD_DIM ** -0.5 * math.log2(math.e)
GROUP = 5
KV_HEADS = 8
BLK = 128
PAIR = 2 * BLK
WIDTH = GROUP * BLK
N_ITEMS = 9
KV_COLS = KV_HEADS * HEAD_DIM
ROW_CHUNKS = (4, 6, 6)
MIB = 1024 * 1024


def rope_tables(positions):
    inv_freq = 1.0 / (ROPE_BASE ** (jnp.arange(0, HEAD_DIM, 2, dtype=jnp.float32) / HEAD_DIM))
    angles = positions.astype(jnp.float32)[:, :, None] * jnp.concatenate([inv_freq, inv_freq])
    sign = jnp.where(jnp.arange(HEAD_DIM) < HEAD_DIM // 2, -1.0, 1.0).astype(jnp.float32)
    return jnp.cos(angles), jnp.sin(angles) * sign


def rotate(vecs, cosv, sinv):
    return (vecs * cosv + pltpu.roll(vecs, HEAD_DIM // 2, 1) * sinv).astype(jnp.bfloat16)


def kv_kernel(chunks, x_ref, wk_ref, wv_ref, cos_ref, sin_ref, *out_refs):
    cosv, sinv = cos_ref[0], sin_ref[0]
    parts = []
    for c in range(0, KV_COLS, PAIR):
        acc = jnp.dot(x_ref[0], wk_ref[:, c:c + PAIR], preferred_element_type=jnp.float32)
        acc = acc.astype(jnp.bfloat16).astype(jnp.float32)
        parts.append((c, jnp.concatenate([rotate(acc[:, h:h + HEAD_DIM], cosv, sinv) for h in range(0, PAIR, HEAD_DIM)], axis=1)))
    for c in range(0, KV_COLS, PAIR):
        acc = jnp.dot(x_ref[0], wv_ref[:, c:c + PAIR], preferred_element_type=jnp.float32)
        parts.append((KV_COLS + c, acc.astype(jnp.bfloat16)))
    step = pl.program_id(0)
    first = 0
    for out_ref, rows in zip(out_refs, chunks):
        @pl.when((step >= first) & (step < first + rows))
        def _(out_ref=out_ref):
            for c, part in parts:
                out_ref[0, :, c:c + PAIR] = part
        first += rows


def project_kv(x, w_key, w_value, cos_t, sin_t, first_row, chunks):
    _, toks, dim = x.shape
    rows = sum(chunks)
    starts = [sum(chunks[:c]) for c in range(len(chunks))]

    def out_map(start, count):
        return lambda n: (jnp.clip(n - start, 0, count - 1), 0, 0)

    return pl.pallas_call(
        functools.partial(kv_kernel, chunks),
        grid=(rows,),
        out_shape=[jax.ShapeDtypeStruct((n, toks, 2 * KV_COLS), jnp.bfloat16) for n in chunks],
        in_specs=[
            pl.BlockSpec((1, toks, dim), lambda n: (n + first_row, 0, 0)),
            pl.BlockSpec((dim, KV_COLS), lambda n: (0, 0), pipeline_mode=pl.Buffered(1)),
            pl.BlockSpec((dim, KV_COLS), lambda n: (0, 0), pipeline_mode=pl.Buffered(1)),
            pl.BlockSpec((1, toks, HEAD_DIM), lambda n: (n + first_row, 0, 0)),
            pl.BlockSpec((1, toks, HEAD_DIM), lambda n: (n + first_row, 0, 0)),
        ],
        out_specs=[pl.BlockSpec((1, toks, 2 * KV_COLS), out_map(s, n)) for s, n in zip(starts, chunks)],
        compiler_params=pltpu.CompilerParams(dimension_semantics=('arbitrary',), vmem_limit_bytes=56 * MIB),
        cost_estimate=pl.CostEstimate(flops=2 * rows * toks * dim * 2 * KV_COLS, bytes_accessed=rows * toks * dim * 2 + dim * KV_COLS * 4, transcendentals=0),
        name='kv_proj',
    )(x, w_key, w_value, cos_t, sin_t)


def attn_kernel(n_steps, q_ref, cos_ref, sin_ref, k_ref, v_ref, o_ref, q_scr, s_scr, m_scr, mc_scr, l_scr, acc_scr):
    me = lax.axis_index('cp')
    step = pl.program_id(0)
    n_back = (17 - me) // 2
    n_front = (me + 2) // 2

    def block_at(ref, b):
        if isinstance(b, int):
            return ref[b, 0, :BLK, :] if b < 8 else ref[15 - b, 0, BLK:, :]
        late = (b >= 8).astype(jnp.int32)
        off = pl.multiple_of(late * BLK, BLK)
        return ref[b + late * (15 - 2 * b), 0, pl.ds(off, BLK), :]

    def pair_at(ref, p):
        return jnp.concatenate([block_at(ref, 2 * p), block_at(ref, 2 * p + 1)], axis=0)

    items = [(0, n_back - 1), (1, n_front - 1), (0, 0), (0, 1), (0, 2), (0, 3)]
    for u in range(3):
        front = (u < n_front - 1).astype(jnp.int32)
        items.append((front, u + (1 - front) * (5 - n_front)))

    def finish(col):
        for half in range(2):
            rows = slice(BLK, 2 * BLK) if half == 0 else slice(0, BLK)
            inv = 1.0 / jnp.sum(l_scr[half], axis=0, keepdims=True)
            out_t = (acc_scr[half] * inv).astype(jnp.bfloat16)
            for g in range(GROUP):
                o_ref[0, rows, pl.ds(pl.multiple_of(col + g * HEAD_DIM, HEAD_DIM), HEAD_DIM)] = out_t[:, g * BLK:(g + 1) * BLK].T

    finish((step % 2) * WIDTH)

    for half in range(2):
        rows = slice(BLK, 2 * BLK) if half == 0 else slice(0, BLK)
        cosv, sinv = cos_ref[0, rows, :], sin_ref[0, rows, :]
        for g in range(GROUP):
            q_scr[half, g * BLK:(g + 1) * BLK, :] = rotate(q_ref[0, rows, g * HEAD_DIM:(g + 1) * HEAD_DIM].astype(jnp.float32), cosv, sinv)

    def weights(t):
        half, pair = items[t]
        e = jnp.exp2(s_scr[t] * SCALE_LOG2 - mc_scr[half])
        part = jnp.sum(e.reshape(PAIR // 8, 8, WIDTH), axis=0)
        return part, jnp.dot(pair_at(v_ref, pair).T, e.astype(jnp.bfloat16), preferred_element_type=jnp.float32)

    def new_scores(t):
        half, pair = items[t]
        s_new = lax.dot_general(pair_at(k_ref, pair), q_scr[half], (((1,), (1,)), ((), ())), preferred_element_type=jnp.float32)
        if t < 2:
            q_blk = 15 - me if t == 0 else me
            key_tok = lax.broadcasted_iota(jnp.int32, (PAIR, BLK), 0) + pair * PAIR
            q_tok = lax.broadcasted_iota(jnp.int32, (PAIR, BLK), 1) + q_blk * BLK
            keep = jnp.concatenate([key_tok <= q_tok] * GROUP, axis=1)
            s_new = jnp.where(keep, s_new, MASK_FILL)
        s_scr[t] = s_new
        return jnp.max(s_new.reshape(PAIR // 8, 8, WIDTH), axis=0)

    l_sum, acc, top = [None, None], [None, None], [None, None]
    for t in range(6):
        half = items[t][0]
        part, pv = weights(t)
        l_sum[half] = part if l_sum[half] is None else l_sum[half] + part
        acc[half] = pv if acc[half] is None else acc[half] + pv
        peak = new_scores(t)
        top[half] = peak if top[half] is None else jnp.maximum(top[half], peak)
    for half in range(2):
        l_scr[half], acc_scr[half], m_scr[half] = l_sum[half], acc[half], top[half]
    for t in range(6, N_ITEMS):
        half = items[t][0]
        part, pv = weights(t)
        l_scr[half] += part
        acc_scr[half] += pv
        m_scr[half] = jnp.maximum(m_scr[half], new_scores(t))
    for half in range(2):
        mc_scr[half] = jnp.max(m_scr[half], axis=0, keepdims=True) * SCALE_LOG2

    @pl.when(step == n_steps)
    def _():
        finish(WIDTH)


def attention(q, cos_t, sin_t, kv_all, first_row):
    rows = kv_all.shape[1]
    toks = q.shape[1]
    n_steps = rows * KV_HEADS

    def cur(n):
        m = jnp.minimum(n, n_steps - 1)
        return m // KV_HEADS, m % KV_HEADS

    def prev(n, back=1):
        m = jnp.maximum(n - back, 0)
        return m // KV_HEADS, m % KV_HEADS

    flops = n_steps * N_ITEMS * 4 * PAIR * WIDTH * HEAD_DIM
    return pl.pallas_call(
        functools.partial(attn_kernel, n_steps),
        grid=(n_steps + 1,),
        out_shape=jax.ShapeDtypeStruct((rows,) + q.shape[1:], jnp.bfloat16),
        in_specs=[
            pl.BlockSpec((1, toks, WIDTH), lambda n: (cur(n)[0] + first_row, 0, cur(n)[1])),
            pl.BlockSpec((1, toks, HEAD_DIM), lambda n: (cur(n)[0] + first_row, 0, 0)),
            pl.BlockSpec((1, toks, HEAD_DIM), lambda n: (cur(n)[0] + first_row, 0, 0)),
            pl.BlockSpec((8, 1, toks, HEAD_DIM), lambda n: (0, cur(n)[0], 0, cur(n)[1])),
            pl.BlockSpec((8, 1, toks, HEAD_DIM), lambda n: (0, prev(n)[0], 0, KV_HEADS + prev(n)[1])),
        ],
        out_specs=pl.BlockSpec((1, toks, 2 * WIDTH), lambda n: (prev(n, 2)[0], 0, prev(n, 2)[1] // 2)),
        scratch_shapes=[
            pltpu.VMEM((2, WIDTH, HEAD_DIM), jnp.bfloat16),
            pltpu.VMEM((N_ITEMS, PAIR, WIDTH), jnp.float32),
            pltpu.VMEM((2, 8, WIDTH), jnp.float32),
            pltpu.VMEM((2, 1, WIDTH), jnp.float32),
            pltpu.VMEM((2, 8, WIDTH), jnp.float32),
            pltpu.VMEM((2, HEAD_DIM, WIDTH), jnp.float32),
        ],
        compiler_params=pltpu.CompilerParams(dimension_semantics=('arbitrary',), vmem_limit_bytes=40 * MIB),
        cost_estimate=pl.CostEstimate(flops=flops, bytes_accessed=rows * toks * (16 * 2 * KV_COLS + 4 * 5120), transcendentals=flops // (4 * HEAD_DIM)),
        name='attn',
    )(q, cos_t, sin_t, kv_all, kv_all)


def unset(shape):
    return pl.pallas_call(
        lambda out_ref: None,
        out_shape=jax.ShapeDtypeStruct(shape, jnp.bfloat16),
        out_specs=pl.BlockSpec(memory_space=pl.ANY),
        name='unset',
    )()


def solution(mesh):
    row_spec = P('data', 'cp', None)
    rep_spec = P(None, None)

    def local_block(x, pos, w_query, w_key, w_value, w_out):
        cos_t, sin_t = rope_tables(pos)
        kv = project_kv(x, w_key, w_value, cos_t, sin_t, 0, ROW_CHUNKS[:1])
        x, kv = lax.optimization_barrier((x, kv))
        kv += project_kv(x, w_key, w_value, cos_t, sin_t, ROW_CHUNKS[0], ROW_CHUNKS[1:])
        gathered = [lax.all_gather(part, 'cp') for part in kv]
        x, kv = lax.optimization_barrier((x, kv))
        q = jnp.einsum('bte,ed->btd', x, w_query, preferred_element_type=jnp.float32).astype(jnp.bfloat16)
        y = unset(x.shape)
        first = 0
        for kv_all in gathered:
            span = slice(first, first + kv_all.shape[1])
            o = attention(q, cos_t, sin_t, kv_all, first)
            part = jnp.einsum('btd,de->bte', o, w_out, preferred_element_type=jnp.float32)
            y = y.at[span].set((x[span].astype(jnp.float32) + part).astype(jnp.bfloat16))
            q, y = lax.optimization_barrier((q, y))
            first = span.stop
        return y

    return jax.shard_map(local_block, mesh=mesh, in_specs=(row_spec, P('data', 'cp'), rep_spec, rep_spec, rep_spec, rep_spec), out_specs=row_spec, check_vma=False)
```

```python
import functools
import math

import jax
import jax.numpy as jnp
from jax import lax
from jax.experimental import pallas as pl
from jax.experimental.pallas import tpu as pltpu
from jax.sharding import PartitionSpec as P

HEAD_DIM = 128
ROPE_BASE = 500000
MASK_FILL = -1e30
SCALE_LOG2 = HEAD_DIM ** -0.5 * math.log2(math.e)
GROUP = 5
KV_HEADS = 8
BLK = 128
PAIR = 2 * BLK
WIDTH = GROUP * BLK
N_BLOCKS = 17
ROWS = 2
KV_COLS = KV_HEADS * HEAD_DIM
ROW_CHUNKS = (6, 6, 4)
MIB = 1024 * 1024


def rope_tables(positions):
    inv_freq = 1.0 / (ROPE_BASE ** (jnp.arange(0, HEAD_DIM, 2, dtype=jnp.float32) / HEAD_DIM))
    angles = positions.astype(jnp.float32)[:, :, None] * jnp.concatenate([inv_freq, inv_freq])
    sign = jnp.where(jnp.arange(HEAD_DIM) < HEAD_DIM // 2, -1.0, 1.0).astype(jnp.float32)
    return jnp.cos(angles), jnp.sin(angles) * sign


def rotate(vecs, cosv, sinv):
    return (vecs * cosv + pltpu.roll(vecs, HEAD_DIM // 2, 1) * sinv).astype(jnp.bfloat16)


def turn_into(out_ref, raw_ref, cos_ref, sin_ref, c):
    for h in range(c, c + PAIR, HEAD_DIM):
        vecs = raw_ref[:, h:h + HEAD_DIM].astype(jnp.float32)
        out_ref[:, :, h:h + HEAD_DIM] = rotate(vecs, flat(cos_ref), flat(sin_ref)).reshape(out_ref.shape[:2] + (HEAD_DIM,))


def flat(ref):
    rows, toks, cols = ref.shape
    return ref[...].reshape(rows * toks, cols)


def kv_kernel(chunks, x_ref, wk_ref, wv_ref, cos_ref, sin_ref, *refs):
    out_refs, (raw_scr,) = refs[:len(chunks)], refs[len(chunks):]
    step = pl.program_id(0)
    first = 0
    for out_ref, count in zip(out_refs, chunks):
        @pl.when((step >= first) & (step < first + count // ROWS))
        def _(out_ref=out_ref):
            for c in range(0, KV_COLS, PAIR):
                raw_scr[:, c:c + PAIR] = jnp.dot(flat(x_ref), wk_ref[:, c:c + PAIR], preferred_element_type=jnp.float32).astype(jnp.bfloat16)
            for c in range(0, KV_COLS, PAIR):
                turn_into(out_ref, raw_scr, cos_ref, sin_ref, c)
                acc = jnp.dot(flat(x_ref), wv_ref[:, c:c + PAIR], preferred_element_type=jnp.float32).astype(jnp.bfloat16)
                out_ref[:, :, KV_COLS + c:KV_COLS + c + PAIR] = acc.reshape(out_ref.shape[:2] + (PAIR,))
        first += count // ROWS


def project_kv(x, w_key, w_value, cos_t, sin_t, first_row, chunks):
    _, toks, dim = x.shape
    total = sum(chunks)
    starts = [sum(chunks[:c]) for c in range(len(chunks))]

    def block(cols):
        return pl.BlockSpec((ROWS, toks, cols), lambda n: (n + first_row // ROWS, 0, 0))

    weights = pl.BlockSpec((dim, KV_COLS), lambda n: (0, 0), pipeline_mode=pl.Buffered(1))

    def out_map(start, count):
        return lambda n: (jnp.clip(n - start // ROWS, 0, count // ROWS - 1), 0, 0)

    return pl.pallas_call(
        functools.partial(kv_kernel, chunks),
        grid=(total // ROWS,),
        out_shape=[jax.ShapeDtypeStruct((n, toks, 2 * KV_COLS), jnp.bfloat16) for n in chunks],
        in_specs=[block(dim), weights, weights, block(HEAD_DIM), block(HEAD_DIM)],
        out_specs=[pl.BlockSpec((ROWS, toks, 2 * KV_COLS), out_map(s, n)) for s, n in zip(starts, chunks)],
        scratch_shapes=[pltpu.VMEM((ROWS * toks, KV_COLS), jnp.bfloat16)],
        compiler_params=pltpu.CompilerParams(dimension_semantics=('arbitrary',), vmem_limit_bytes=56 * MIB),
        cost_estimate=pl.CostEstimate(flops=2 * total * toks * dim * 2 * KV_COLS, bytes_accessed=total * toks * dim * 2 + dim * KV_COLS * 4, transcendentals=0),
        name='kv_proj',
    )(x, w_key, w_value, cos_t, sin_t)


def q_kernel(n_tiles, x_ref, w_ref, cos_ref, sin_ref, q_ref, raw_scr):
    step = pl.program_id(0)

    @pl.when(step < n_tiles)
    def _():
        for c in range(0, q_ref.shape[2], PAIR):
            turn_into(q_ref, raw_scr, cos_ref, sin_ref, c)
            raw_scr[:, c:c + PAIR] = jnp.dot(flat(x_ref), w_ref[:, c:c + PAIR], preferred_element_type=jnp.float32).astype(jnp.bfloat16)

    @pl.when(step == n_tiles)
    def _():
        for c in range(0, q_ref.shape[2], PAIR):
            turn_into(q_ref, raw_scr, cos_ref, sin_ref, c)


def project_q(x, w_query, cos_t, sin_t):
    rows, toks, dim = x.shape
    cols, group = 512, 2 * ROWS
    across = w_query.shape[1] // cols
    n_tiles = rows // group * across

    def cur(n):
        m = jnp.minimum(n, n_tiles - 1)
        return m // across, m % across

    def prev(n):
        m = jnp.maximum(n - 1, 0)
        return m // across, m % across

    table = pl.BlockSpec((group, toks, HEAD_DIM), lambda n: (prev(n)[0], 0, 0))
    return pl.pallas_call(
        functools.partial(q_kernel, n_tiles),
        grid=(n_tiles + 1,),
        out_shape=jax.ShapeDtypeStruct((rows, toks, w_query.shape[1]), jnp.bfloat16),
        in_specs=[
            pl.BlockSpec((group, toks, dim), lambda n: (cur(n)[0], 0, 0)),
            pl.BlockSpec((dim, cols), lambda n: (0, cur(n)[1])),
            table, table,
        ],
        out_specs=pl.BlockSpec((group, toks, cols), lambda n: (prev(n)[0], 0, prev(n)[1])),
        scratch_shapes=[pltpu.VMEM((group * toks, cols), jnp.bfloat16)],
        compiler_params=pltpu.CompilerParams(dimension_semantics=('arbitrary',), vmem_limit_bytes=56 * MIB),
        cost_estimate=pl.CostEstimate(flops=2 * rows * toks * dim * w_query.shape[1], bytes_accessed=2 * x.size * 2 + w_query.size * 2, transcendentals=0),
        name='q_proj',
    )(x, w_query, cos_t, sin_t)


def attn_kernel(n_steps, q_ref, k_ref, v_ref, o_ref, s_scr, m_scr, mc_scr, l_scr, acc_scr, l_done, acc_done):
    me = lax.axis_index('cp')
    step = pl.program_id(0)

    def block_at(ref, b):
        if isinstance(b, int):
            return ref[b, 0, :BLK, :] if b < 8 else ref[15 - b, 0, BLK:, :]
        late = (b >= 8).astype(jnp.int32)
        off = pl.multiple_of(late * BLK, BLK)
        return ref[b + late * (15 - 2 * b), 0, pl.ds(off, BLK), :]

    def keys_at(ref, blocks):
        return jnp.concatenate([block_at(ref, b) for b in blocks], axis=0)

    odd = me % 2
    items = [(0, (15 - me, 0, 1)), (1, (me,)), (odd, (14 - me + odd * (2 * me - 15),)), (0, (2, 3)), (0, (4, 5)), (0, (6, 7))]
    for u in range(3):
        front = (u < me // 2).astype(jnp.int32)
        pair = u + (1 - front) * (4 - me // 2)
        items.append((front, (2 * pair, 2 * pair + 1)))
    ends = [0]
    for _, blocks in items:
        ends.append(ends[-1] + BLK * len(blocks))

    def half_rows(half):
        return slice(BLK, 2 * BLK) if half == 0 else slice(0, BLK)

    def queries(half):
        off = (1 - half) * BLK
        off = off if isinstance(off, int) else pl.multiple_of(off, BLK)
        return jnp.concatenate([q_ref[0, pl.ds(off, BLK), g * HEAD_DIM:(g + 1) * HEAD_DIM] for g in range(GROUP)], axis=0)

    def finish(l_in, acc_in, col):
        for half in range(2):
            inv = 1.0 / jnp.sum(l_in[half], axis=0, keepdims=True)
            out_t = (acc_in[half] * inv).astype(jnp.bfloat16)
            for g in range(GROUP):
                o_ref[0, half_rows(half), pl.ds(pl.multiple_of(col + g * HEAD_DIM, HEAD_DIM), HEAD_DIM)] = out_t[:, g * BLK:(g + 1) * BLK].T

    l_done[...] = l_scr[...]
    acc_done[...] = acc_scr[...]
    for t, (half, blocks) in enumerate(items):
        n_keys = ends[t + 1] - ends[t]
        span = slice(ends[t], ends[t + 1])
        vt = keys_at(v_ref, blocks).T
        e = jnp.exp2(s_scr[span] * SCALE_LOG2 - mc_scr[half])
        part = jnp.sum(e.reshape(n_keys // 8, 8, WIDTH), axis=0)
        pv = jnp.dot(vt, e.astype(jnp.bfloat16), preferred_element_type=jnp.float32)
        if t < 2:
            l_scr[half], acc_scr[half] = part, pv
        else:
            l_scr[half] += part
            acc_scr[half] += pv
        s_new = lax.dot_general(keys_at(k_ref, blocks), queries(half), (((1,), (1,)), ((), ())), preferred_element_type=jnp.float32)
        if t < 2:
            keep = lax.broadcasted_iota(jnp.int32, (BLK, BLK), 0) <= lax.broadcasted_iota(jnp.int32, (BLK, BLK), 1)
            masked = jnp.where(jnp.concatenate([keep] * GROUP, axis=1), s_new[:BLK], MASK_FILL)
            s_new = jnp.concatenate([masked, s_new[BLK:]], axis=0) if n_keys > BLK else masked
        s_scr[span] = s_new
        peak = jnp.max(s_new.reshape(n_keys // 8, 8, WIDTH), axis=0)
        m_scr[half] = peak if t < 2 else jnp.maximum(m_scr[half], peak)
        if t == 8:
            finish(l_done, acc_done, (step % 2) * WIDTH)
    for half in range(2):
        mc_scr[half] = jnp.max(m_scr[half], axis=0, keepdims=True) * SCALE_LOG2

    @pl.when(step == n_steps)
    def _():
        finish(l_scr, acc_scr, WIDTH)


def attention(q, kv_all, first_row):
    rows = kv_all.shape[1]
    toks = q.shape[1]
    n_steps = rows * KV_HEADS

    def head_of(n):
        m = jnp.clip(n, 0, n_steps - 1)
        return m // KV_HEADS, m % KV_HEADS

    flops = n_steps * N_BLOCKS * 4 * BLK * WIDTH * HEAD_DIM
    return pl.pallas_call(
        functools.partial(attn_kernel, n_steps),
        grid=(n_steps + 1,),
        out_shape=jax.ShapeDtypeStruct((rows,) + q.shape[1:], jnp.bfloat16),
        in_specs=[
            pl.BlockSpec((1, toks, WIDTH), lambda n: (head_of(n)[0] + first_row, 0, head_of(n)[1])),
            pl.BlockSpec((8, 1, toks, HEAD_DIM), lambda n: (0, head_of(n)[0], 0, head_of(n)[1])),
            pl.BlockSpec((8, 1, toks, HEAD_DIM), lambda n: (0, head_of(n - 1)[0], 0, KV_HEADS + head_of(n - 1)[1])),
        ],
        out_specs=pl.BlockSpec((1, toks, 2 * WIDTH), lambda n: (head_of(n - 2)[0], 0, head_of(n - 2)[1] // 2)),
        scratch_shapes=[
            pltpu.VMEM((N_BLOCKS * BLK, WIDTH), jnp.float32),
            pltpu.VMEM((2, 8, WIDTH), jnp.float32),
            pltpu.VMEM((2, 1, WIDTH), jnp.float32),
            pltpu.VMEM((2, 8, WIDTH), jnp.float32),
            pltpu.VMEM((2, HEAD_DIM, WIDTH), jnp.float32),
            pltpu.VMEM((2, 8, WIDTH), jnp.float32),
            pltpu.VMEM((2, HEAD_DIM, WIDTH), jnp.float32),
        ],
        compiler_params=pltpu.CompilerParams(dimension_semantics=('arbitrary',), vmem_limit_bytes=58 * MIB),
        cost_estimate=pl.CostEstimate(flops=flops, bytes_accessed=rows * toks * (16 * 2 * KV_COLS + 4 * 5120), transcendentals=flops // (4 * HEAD_DIM)),
        name='attn',
    )(q, kv_all, kv_all)


def unset(shape):
    return pl.pallas_call(
        lambda out_ref: None,
        out_shape=jax.ShapeDtypeStruct(shape, jnp.bfloat16),
        out_specs=pl.BlockSpec(memory_space=pl.ANY),
        name='unset',
    )()


def solution(mesh):
    row_spec = P('data', 'cp', None)
    rep_spec = P(None, None)

    def local_block(x, pos, w_query, w_key, w_value, w_out):
        cos_t, sin_t = rope_tables(pos)
        kv = project_kv(x, w_key, w_value, cos_t, sin_t, 0, ROW_CHUNKS[:1])
        x, kv = lax.optimization_barrier((x, kv))
        kv += project_kv(x, w_key, w_value, cos_t, sin_t, ROW_CHUNKS[0], ROW_CHUNKS[1:])
        gathered = [lax.all_gather(part, 'cp') for part in kv]
        x, kv = lax.optimization_barrier((x, kv))
        q = project_q(x, w_query, cos_t, sin_t)
        y, first = unset(x.shape), 0
        for kv_all in gathered:
            span = slice(first, first + kv_all.shape[1])
            o = attention(q, kv_all, first)
            part = jnp.einsum('btd,de->bte', o, w_out, preferred_element_type=jnp.float32)
            y = y.at[span].set((x[span].astype(jnp.float32) + part).astype(jnp.bfloat16))
            q, y = lax.optimization_barrier((q, y))
            first = span.stop
        return y

    return jax.shard_map(local_block, mesh=mesh, in_specs=(row_spec, P('data', 'cp'), rep_spec, rep_spec, rep_spec, rep_spec), out_specs=row_spec, check_vma=False)
```
